512 devices in a mesh: parts: 2 (over y), pix: 32 (over z), par: 8 (over x, core).
Axes of the slice: x: 4, y: 2, z: 32, core: 2. Of those that a mesh axis runs over, the one named last changes fastest.
The devices are a block of a 4x8x32 slice.
Arguments:
- green_matrix: bfloat16 [36864, 16384], P('pix', 'par'), may hold values from -0.046875 to 0.046875
- observed: bfloat16 [64, 36864], P('parts', 'pix'), parts along dimension 0, may hold values from -1000 to 1000
Outputs:
- solution: float32 [64, 16384], P('parts', 'par'), parts along dimension 0
- residual: float32 [64, 36864], P('parts', 'pix'), parts along dimension 0
The draws below stay inside these ranges and needn't reach their ends.
There are 2 independent parts, one for each index of `parts`. The reference program is written for one: setup_inputs(seed, part) draws one part's arguments, and reference() takes and returns one part's arrays. A program takes and returns all parts, laid end to end along the dimension named above; an argument that names none is the same for every part. Nothing has to cross between parts.
All inputs are finite; a program needn't handle non-finite values.
Results may differ from the reference program's by a relative error of at most 0.0038.
Values may be sent and summed in bfloat16 or wider, within the bound.
A program may use at most 64 MiB of HBM per device.

```python
import math
import jax
import jax.numpy as jnp
from jax import lax

GRID = 128
PARAMS = 16384
SETS = 32
PIXELS = 36864
ITERS = 5


def draw_green_matrix(key, part):
    keys = jax.random.split(jax.random.fold_in(key, 29), 4)
    base = jnp.clip(jax.random.normal(keys[0], (PIXELS, PARAMS), jnp.float32), -6.0, 6.0)
    column_scale = jnp.exp(jax.random.uniform(keys[1], (1, PARAMS), jnp.float32, -2.5, 0.0))
    left = jax.random.normal(keys[2], (PIXELS, 3), jnp.float32)
    right = jax.random.normal(keys[3], (3, PARAMS), jnp.float32)
    common = left[:, 0:1] * right[0:1, :] + left[:, 1:2] * right[1:2, :] + left[:, 2:3] * right[2:3, :]
    common = common / math.sqrt(3.0)
    place = jnp.arange(PARAMS, dtype=jnp.float32)[None, :] / PARAMS - 1.0
    rising = jnp.exp(math.log(3.0) * place)
    value = (base + 0.06 * common) * column_scale * rising * (2.2 / GRID)
    bound = 6.0 / GRID
    return jnp.clip(value, -bound, bound).astype(jnp.bfloat16)


def draw_observed(key, part):
    keys = jax.random.split(jax.random.fold_in(key, 71), 3)
    position = jnp.arange(PIXELS, dtype=jnp.float32) / PIXELS
    base = jnp.clip(jax.random.normal(keys[0], (SETS, PIXELS), jnp.float32), -6.0, 6.0)
    rising = jnp.exp(math.log(3.0) * position)[None, :]
    row_scale = jnp.exp(jax.random.uniform(keys[1], (1, PIXELS), jnp.float32, math.log(0.5), math.log(5.0)))
    set_scale = jnp.exp(jax.random.uniform(keys[2], (SETS, 1), jnp.float32, math.log(0.3), math.log(3.0)))
    return (base * rising * row_scale * set_scale).astype(jnp.bfloat16)


def setup_inputs(seed: int = 0, part: int = 0) -> dict:
    seeds = jax.random.split(jax.random.key(seed), 3)
    own_keys = jax.random.split(jax.random.fold_in(seeds[2], part), 3)
    green_matrix = draw_green_matrix(jax.random.fold_in(seeds[2], 71), part)
    observed = draw_observed(jax.random.fold_in(jax.random.fold_in(seeds[2], part), 71), part)
    return {"green_matrix": green_matrix, "observed": observed}


def smooth(values):
    set_count = values.shape[0]
    tiles = values.reshape(set_count, GRID, GRID)
    padded = jnp.pad(tiles, ((0, 0), (1, 1), (1, 1)))
    beside_all = padded[:, 2:, 1:-1] + padded[:, :-2, 1:-1] + padded[:, 1:-1, 2:] + padded[:, 1:-1, :-2]
    return (0.25 * (4.0 * tiles - beside_all)).reshape(set_count, GRID * GRID)


def reference(green_matrix, observed):
    residual = observed.astype(jnp.float32)
    gradient = jnp.dot(observed, green_matrix, preferred_element_type=jnp.float32)
    grad_sq = jnp.sum(gradient * gradient, axis=1)
    direction = gradient
    solution = jnp.zeros((SETS, GRID * GRID), jnp.float32)
    smooth_res = jnp.zeros((SETS, GRID * GRID), jnp.float32)
    for sweep in range(ITERS):
        rounded = direction.astype(jnp.bfloat16)
        image = lax.dot_general(rounded, green_matrix, (((1,), (1,)), ((), ())), preferred_element_type=jnp.float32)
        smoothed = smooth(lax.optimization_barrier(rounded).astype(jnp.float32))
        curvature = jnp.sum(image * image, axis=1) + jnp.sum(smoothed * smoothed, axis=1)
        step_len = (grad_sq / curvature)[:, None]
        solution = solution + step_len * direction
        residual = residual - step_len * image
        smooth_res = smooth_res - step_len * smoothed
        if sweep + 1 < ITERS:
            gradient = jnp.dot(residual.astype(jnp.bfloat16), green_matrix, preferred_element_type=jnp.float32) + smooth(smooth_res)
            fresh_sq = jnp.sum(gradient * gradient, axis=1)
            direction = gradient + (fresh_sq / grad_sq)[:, None] * direction
            grad_sq = fresh_sq
    return solution, residual
```

```python
import functools

import jax
import jax.numpy as jnp
from jax import lax
from jax.experimental import pallas as pl
from jax.experimental.pallas import tpu as pltpu
from jax.sharding import PartitionSpec as P

GRID = 128
ITERS = 5
WINDOW = 8
NEAR = (4, -3, 3, -2, 2, -1, 1)
F32 = jnp.float32
BF16 = jnp.bfloat16
MESH = pl.DeviceIdType.MESH


def row_sums(value, eye):
    column = jnp.sum(value, axis=1, keepdims=True)
    return jnp.sum(jnp.where(eye, column, 0.0), axis=0, keepdims=True)


def to_column(row, eye):
    return jnp.sum(jnp.where(eye, row, 0.0), axis=1, keepdims=True)


def kernel(
    n_pix, n_par, green, observed, sol_out, res_out,
    gmat, grad, near_send, near_recv, near_low, near_low_recv, own_part, wide_send, wide_recv,
    wide_low, wide_low_recv, rows_near, rows_wide,
    near_grad, halo, direction, smooth1, smooth2, solution, residual, image, image_bf,
    partial, pair_recv, chip_buf, half_send, half_recv, fresh_rows, smooth_rows, final_rows, row_send,
    g_sem, as_sem, ar_sem, bs_sem, br_sem, cs_sem, cr_sem, hs_sem, hr_sem, xs_sem, x1r_sem, x2r_sem,
    x3r_sem, fs_sem, fr_sem, ss_sem, sr_sem, zs_sem, zr_sem, ars_sem, arr_sem, brs_sem, brr_sem,
    als_sem, alr_sem, bls_sem, blr_sem,
):
    sets = observed.shape[0]
    pixels = observed.shape[1]
    chunk = gmat.shape[2]
    rows_per = chunk // GRID
    blocks = n_pix // WINDOW
    rows = direction.shape[0] - 2 * rows_per
    half = sets // 2
    z = lax.axis_index("pix")
    par = lax.axis_index("par")
    core = lax.rem(par, 2)
    chip = lax.div(par, 2)
    chips = n_par // 2
    mate = par + 1 - 2 * core
    own_class = lax.rem(z, WINDOW)
    own_block = lax.div(z, WINDOW)

    def at_pix(offset):
        return {"pix": lax.rem(z + (offset + n_pix), n_pix)}

    def at_par(offset):
        return {"par": lax.rem(par + offset, n_par)}

    def class_at(offset):
        return lax.rem(z + (offset + n_pix), WINDOW)

    def remote(src, dst, send, recv, device):
        return pltpu.make_async_remote_copy(
            src_ref=src, dst_ref=dst, send_sem=send, recv_sem=recv, device_id=device, device_id_type=MESH
        )

    loads = []
    for index in range(WINDOW):
        load = pltpu.make_async_copy(
            green.at[:, pl.ds(index * chunk, chunk)], gmat.at[index], g_sem.at[index]
        )
        load.start()
        loads.append(load)

    halo[...] = jnp.zeros_like(halo)
    smooth_rows[...] = jnp.zeros_like(smooth_rows)
    barrier = pltpu.get_barrier_semaphore()
    for offset in range(1, n_pix):
        pl.semaphore_signal(barrier, inc=1, device_id=at_pix(offset), device_id_type=MESH)
    for offset in range(1, n_par):
        pl.semaphore_signal(barrier, inc=1, device_id=at_par(offset), device_id_type=MESH)

    lane = lax.broadcasted_iota(jnp.int32, (sets, GRID), 1)
    eye = lane == lax.broadcasted_iota(jnp.int32, (sets, GRID), 0)
    first_lane = lane == 0
    last_lane = lane == GRID - 1

    direction[...] = jnp.zeros_like(direction)
    smooth2[...] = jnp.zeros_like(smooth2)
    smooth1[...] = jnp.zeros_like(smooth1)
    solution[...] = jnp.zeros_like(solution)
    image[...] = jnp.zeros_like(image)
    grad[...] = jnp.zeros_like(grad)
    image_bf[...] = observed[...]
    residual[...] = observed[...].astype(F32)
    for load in loads:
        load.wait()
    pl.semaphore_wait(barrier, n_pix - 1 + n_par - 1)

    def all_par(rows_ref, row, slot_sem, send_sem, index):
        row_send[index] = row
        rows_ref[par] = row
        for offset in range(1, n_par):
            remote(
                row_send.at[index], rows_ref.at[par], send_sem, slot_sem, at_par(offset)
            ).start()

    def wait_rows(rows_ref, sem, count):
        part = rows_ref.at[pl.ds(0, count)]
        remote(part, part, sem, sem, at_par(1)).wait_recv()

    def neighbours_sum(field, row):
        here = field[row]
        left = jnp.where(first_lane, 0.0, pltpu.roll(here, 1, 1))
        right = jnp.where(last_lane, 0.0, pltpu.roll(here, GRID - 1, 1))
        return here, left + right

    def sum_par(rows_ref):
        total = rows_ref[0]
        for index in range(1, n_par):
            total = total + rows_ref[index]
        return total

    def sweep_body(sweep, grad_sq):
        parity = lax.rem(sweep, 2)
        started = sweep > 0

        lhs = image_bf[...]
        for slot, offset in enumerate(NEAR):
            product = jnp.dot(lhs, gmat[class_at(offset)], preferred_element_type=F32)
            rounded = product.astype(BF16)
            near_send[slot] = rounded
            remote(near_send.at[slot], near_recv.at[slot], as_sem, ar_sem, at_pix(offset)).start()

            @pl.when(jnp.logical_not(started))
            def _():
                near_low[slot] = (product - rounded.astype(F32)).astype(BF16)
                remote(
                    near_low.at[slot], near_low_recv.at[slot], als_sem, alr_sem, at_pix(offset)
                ).start()

        value = image[...]
        image_row = row_sums(value * value, eye)
        row_send[2] = image_row
        rows_near[len(NEAR)] = image_row
        for slot, offset in enumerate(NEAR):
            remote(row_send.at[2], rows_near.at[slot], ars_sem, arr_sem, at_pix(offset)).start()
        total = jnp.dot(lhs, gmat[own_class], preferred_element_type=F32)
        remote(near_recv, near_recv, ar_sem, ar_sem, at_pix(1)).wait_recv()
        for slot in range(len(NEAR)):
            total = total + near_recv[slot].astype(F32)
        own_part[...] = total

        @pl.when(jnp.logical_not(started))
        def _():
            remote(near_low_recv, near_low_recv, als_sem, alr_sem, at_pix(1)).wait_recv()
            more = near_low_recv[0].astype(F32)
            for slot in range(1, len(NEAR)):
                more = more + near_low_recv[slot].astype(F32)
            own_part[...] += more

        total = own_part[...]
        rounded = total.astype(BF16)
        wide_send[...] = rounded
        wide_recv[parity, 0] = rounded
        order = [blocks // 2] + [b for b in range(1, blocks) if b != blocks // 2]
        for block in order:
            remote(
                wide_send, wide_recv.at[parity, blocks - block], bs_sem, br_sem.at[parity],
                at_pix(block * WINDOW),
            ).start()

        @pl.when(jnp.logical_not(started))
        def _():
            low_part = (total - rounded.astype(F32)).astype(BF16)
            wide_low[...] = low_part
            wide_low_recv[0] = low_part
            for block in order:
                remote(
                    wide_low, wide_low_recv.at[blocks - block], bls_sem, blr_sem,
                    at_pix(block * WINDOW),
                ).start()

        part = rows_near.at[pl.ds(0, len(NEAR))]
        remote(part, part, arr_sem, arr_sem, at_pix(1)).wait_recv()
        for slot in range(WINDOW):
            rows_wide[parity, 0, slot] = rows_near[slot]
        for block in order:
            remote(
                rows_wide.at[parity, 0], rows_wide.at[parity, blocks - block], brs_sem, brr_sem.at[parity],
                at_pix(block * WINDOW),
            ).start()

        @pl.when(started)
        def _():
            wait_rows(smooth_rows, sr_sem, n_par - 1)

        smooth_sq = sum_par(smooth_rows)

        part = rows_wide.at[parity, pl.ds(0, blocks - 1)]
        remote(part, part, brs_sem, brr_sem.at[parity], at_pix(1)).wait_recv()
        image_sq = canonical_rows(parity)
        step_row = jnp.where(started, grad_sq / (image_sq + smooth_sq), -1.0)
        step = to_column(step_row, eye)

        part = wide_recv.at[parity, pl.ds(0, blocks - 1)]
        remote(part, part, bs_sem, br_sem.at[parity], at_pix(1)).wait_recv()
        total = None
        for block in range(blocks):
            term = wide_recv[parity, lax.rem(block - own_block + blocks, blocks)].astype(F32)
            total = term if total is None else total + term
        own_part[...] = total

        @pl.when(jnp.logical_not(started))
        def _():
            part = wide_low_recv.at[pl.ds(0, blocks - 1)]
            remote(part, part, bls_sem, blr_sem, at_pix(1)).wait_recv()
            more = None
            for block in range(blocks):
                place = lax.rem(block - own_block + blocks, blocks)
                term = wide_low_recv[place].astype(F32)
                more = term if more is None else more + term
            own_part[...] += more
            remote(near_low, near_low, als_sem, alr_sem, at_pix(1)).wait_send()
            remote(part, part, bls_sem, blr_sem, at_pix(1)).wait_send()

        total = own_part[...]
        for index in range(rows_per):
            cut = slice(index * GRID, (index + 1) * GRID)
            full = total[:, cut] + smooth2[own_class * rows_per + index]
            grad[:, cut] = grad[:, cut] - step * full
        rounded = grad[...].astype(BF16)
        near_grad[own_class] = rounded
        for offset in NEAR:
            remote(
                near_grad.at[own_class], near_grad.at[own_class], cs_sem, cr_sem.at[offset + 3],
                at_pix(-offset),
            ).start()

        residual[...] = residual[...] - step * image[...]

        def taken(index):
            block = near_grad[index]
            value = block.astype(F32)
            return (
                lax.dot_general(
                    block, gmat[index], (((1,), (1,)), ((), ())), preferred_element_type=F32
                ),
                value * value,
            )

        product, squares = taken(own_class)
        partial[...] = product
        for offset in (1, -1, 2, -2, 3, -3, 4):
            remote(
                near_grad.at[0], near_grad.at[0], cs_sem, cr_sem.at[offset + 3], at_pix(1)
            ).wait_recv()
            product, more = taken(class_at(offset))
            partial[...] += product
            squares = squares + more
        all_par(fresh_rows, row_sums(squares, eye), fr_sem, fs_sem, 0)
        away = remote(
            partial.at[pl.ds(pl.multiple_of((1 - core) * half, half), half)], pair_recv,
            xs_sem.at[0], x1r_sem, {"par": mate},
        )
        away.start()

        low = remote(near_grad.at[0], halo.at[1], hs_sem.at[0], hr_sem.at[1], {"par": lax.rem(par + n_par - 1, n_par)})
        high = remote(near_grad.at[WINDOW - 1], halo.at[0], hs_sem.at[1], hr_sem.at[0], at_par(1))

        @pl.when(par > 0)
        def _():
            low.start()

        @pl.when(par < n_par - 1)
        def _():
            high.start()

        away.wait_recv()
        mine = partial[pl.ds(pl.multiple_of(core * half, half), half)] + pair_recv[...]
        chip_buf[parity, chip] = mine.astype(BF16)
        for offset in (2, 1, 3):
            remote(
                chip_buf.at[parity, chip], chip_buf.at[parity, chip], xs_sem.at[1], x2r_sem.at[parity],
                at_par(2 * offset),
            ).start()

        wait_rows(fresh_rows, fr_sem, n_par - 1)
        fresh_sq = sum_par(fresh_rows)
        ratio_row = jnp.where(started, fresh_sq / grad_sq, 0.0)
        ratio = to_column(ratio_row, eye)
        for row in range(rows):
            old = direction[row + rows_per]
            solution[row] = solution[row] + step * old
            cut = slice(row % rows_per * GRID, (row % rows_per + 1) * GRID)
            new = near_grad[row // rows_per, :, cut].astype(F32)
            direction[row + rows_per] = new + ratio * old

        @pl.when(par < n_par - 1)
        def _():
            low.wait_recv()

        @pl.when(par > 0)
        def _():
            high.wait_recv()

        for index in range(rows_per):
            cut = slice(index * GRID, (index + 1) * GRID)
            direction[index] = halo[0, :, cut].astype(F32) + ratio * direction[index]
            top = rows + rows_per + index
            direction[top] = halo[1, :, cut].astype(F32) + ratio * direction[top]

        squares = None
        for row in range(rows + 2):
            here, beside = neighbours_sum(direction, row + rows_per - 1)
            beside = beside + direction[row + rows_per - 2] + direction[row + rows_per]
            value = here - 0.25 * beside
            if row == 0:
                value = jnp.where(par > 0, value, 0.0)
            elif row == rows + 1:
                value = jnp.where(par < n_par - 1, value, 0.0)
            else:
                squares = value * value if squares is None else squares + value * value
            smooth1[row] = value
        all_par(smooth_rows, row_sums(squares, eye), sr_sem, ss_sem, 1)
        for row in range(rows):
            here, beside = neighbours_sum(smooth1, row + 1)
            smooth2[row] = here - 0.25 * (beside + smooth1[row] + smooth1[row + 2])

        part = chip_buf.at[parity, pl.ds(0, chips - 1)]
        remote(part, part, xs_sem.at[1], x2r_sem.at[parity], at_par(1)).wait_recv()
        total = chip_buf[parity, 0].astype(F32)
        for index in range(1, chips):
            total = total + chip_buf[parity, index].astype(F32)
        my_rows = pl.ds(pl.multiple_of(core * half, half), half)
        their_rows = pl.ds(pl.multiple_of((1 - core) * half, half), half)
        half_send[...] = total
        back = remote(half_send, half_recv, xs_sem.at[2], x3r_sem, {"par": mate})
        back.start()
        partial[my_rows] = total
        away.wait_send()
        back.wait_recv()
        partial[their_rows] = half_recv[...]
        value = partial[...] + ratio * image[...]
        image[...] = value
        image_bf[...] = value.astype(BF16)

        remote(near_send, near_send, as_sem, as_sem, at_pix(1)).wait_send()
        part = rows_near.at[pl.ds(0, len(NEAR))]
        remote(part, part, ars_sem, ars_sem, at_pix(1)).wait_send()
        part = wide_recv.at[parity, pl.ds(0, blocks - 1)]
        remote(part, part, bs_sem, bs_sem, at_pix(1)).wait_send()
        part = rows_wide.at[parity, pl.ds(0, blocks - 1)]
        remote(part, part, brs_sem, brs_sem, at_pix(1)).wait_send()
        remote(near_send, near_send, cs_sem, cs_sem, at_pix(1)).wait_send()
        part = fresh_rows.at[pl.ds(0, n_par - 1)]
        remote(part, part, fs_sem, fs_sem, at_pix(1)).wait_send()
        remote(part, part, ss_sem, ss_sem, at_pix(1)).wait_send()
        part = chip_buf.at[parity, pl.ds(0, chips - 1)]
        remote(part, part, xs_sem.at[1], xs_sem.at[1], at_par(1)).wait_send()
        back.wait_send()

        @pl.when(par > 0)
        def _():
            low.wait_send()

        @pl.when(par < n_par - 1)
        def _():
            high.wait_send()

        return fresh_sq

    def canonical_rows(parity):
        total = None
        for shard in range(n_pix):
            back = lax.rem(shard - z + (2 * n_pix + WINDOW // 2), n_pix)
            block = lax.div(back, WINDOW)
            inside = lax.rem(back, WINDOW)
            row = rows_wide[parity, block, slot_of(inside)]
            total = row if total is None else total + row
        return total

    def slot_of(inside):
        offset = WINDOW // 2 - inside
        slot = len(NEAR)
        for index, value in enumerate(NEAR):
            slot = jnp.where(offset == value, index, slot)
        return slot

    grad_sq = lax.fori_loop(0, ITERS, sweep_body, jnp.zeros((1, GRID), F32))

    value = image[...]
    image_row = row_sums(value * value, eye)
    row_send[2] = image_row
    final_rows[z] = image_row
    for offset in [s * d for d in range(n_pix // 2, 0, -1) for s in (1, -1)][1:]:
        remote(row_send.at[2], final_rows.at[z], zs_sem, zr_sem, at_pix(offset)).start()
    wait_rows(smooth_rows, sr_sem, n_par - 1)
    smooth_sq = sum_par(smooth_rows)
    part = final_rows.at[pl.ds(0, n_pix - 1)]
    remote(part, part, zs_sem, zr_sem, at_pix(1)).wait_recv()
    image_sq = final_rows[0]
    for shard in range(1, n_pix):
        image_sq = image_sq + final_rows[shard]
    step = to_column(grad_sq / (image_sq + smooth_sq), eye)
    for row in range(rows):
        sol_out[:, row * GRID : (row + 1) * GRID] = solution[row] + step * direction[row + rows_per]
    res_out[...] = residual[...] - step * image[...]
    remote(part, part, zs_sem, zs_sem, at_pix(1)).wait_send()


def solution(mesh):
    n_pix, n_par = mesh.shape["pix"], mesh.shape["par"]

    def on_device(green_matrix, observed):
        pixels, cells = green_matrix.shape
        sets = observed.shape[0]
        chunk = cells // WINDOW
        rows = cells // GRID
        extra = chunk // GRID
        blocks = n_pix // WINDOW
        half = sets // 2
        near = len(NEAR)
        dma = pltpu.SemaphoreType.DMA
        vmem = pltpu.VMEM
        return pl.pallas_call(
            functools.partial(kernel, n_pix, n_par),
            out_shape=(
                jax.ShapeDtypeStruct((sets, cells), F32),
                jax.ShapeDtypeStruct((sets, pixels), F32),
            ),
            in_specs=[
                pl.BlockSpec(memory_space=pl.ANY),
                pl.BlockSpec(memory_space=pltpu.VMEM),
            ],
            out_specs=(
                pl.BlockSpec(memory_space=pltpu.VMEM),
                pl.BlockSpec(memory_space=pltpu.VMEM),
            ),
            scratch_shapes=[
                vmem((WINDOW, pixels, chunk), BF16),
                vmem((sets, chunk), F32),
                vmem((near, sets, chunk), BF16),
                vmem((near, sets, chunk), BF16),
                vmem((near, sets, chunk), BF16),
                vmem((near, sets, chunk), BF16),
                vmem((sets, chunk), F32),
                vmem((sets, chunk), BF16),
                vmem((2, blocks, sets, chunk), BF16),
                vmem((sets, chunk), BF16),
                vmem((blocks, sets, chunk), BF16),
                vmem((WINDOW, 1, GRID), F32),
                vmem((2, blocks, WINDOW, 1, GRID), F32),
                vmem((WINDOW, sets, chunk), BF16),
                vmem((2, sets, chunk), BF16),
                vmem((rows + 2 * extra, sets, GRID), F32),
                vmem((rows + 2, sets, GRID), F32),
                vmem((rows, sets, GRID), F32),
                vmem((rows, sets, GRID), F32),
                vmem((sets, pixels), F32),
                vmem((sets, pixels), F32),
                vmem((sets, pixels), BF16),
                vmem((sets, pixels), F32),
                vmem((half, pixels), F32),
                vmem((2, n_par // 2, half, pixels), BF16),
                vmem((half, pixels), F32),
                vmem((half, pixels), F32),
                vmem((n_par, 1, GRID), F32),
                vmem((n_par, 1, GRID), F32),
                vmem((n_pix, 1, GRID), F32),
                vmem((3, 1, GRID), F32),
                dma((WINDOW,)),
                dma, dma,
                dma, dma((2,)),
                dma, dma((WINDOW,)),
                dma((2,)), dma((2,)),
                dma((3,)), dma, dma((2,)), dma,
                dma, dma,
                dma, dma,
                dma, dma,
                dma, dma,
                dma, dma((2,)),
                dma, dma, dma, dma,
            ],
            compiler_params=pltpu.CompilerParams(collective_id=0, has_side_effects=True),
        )(green_matrix, observed)

    return jax.shard_map(
        on_device,
        mesh=mesh,
        in_specs=(P("pix", "par"), P("parts", "pix")),
        out_specs=(P("parts", "par"), P("parts", "pix")),
        check_vma=False,
    )
```

```python
import functools

import jax
import jax.numpy as jnp
from jax import lax
from jax.experimental import pallas as pl
from jax.experimental.pallas import tpu as pltpu
from jax.sharding import PartitionSpec as P

GRID = 128
ITERS = 5
WINDOW = 8
NEAR = (4, -3, 3, -2, 2, -1, 1)
F32 = jnp.float32
BF16 = jnp.bfloat16
MESH = pl.DeviceIdType.MESH


def row_sums(value, eye):
    column = jnp.sum(value, axis=1, keepdims=True)
    return jnp.sum(jnp.where(eye, column, 0.0), axis=0, keepdims=True)


def to_column(row, eye):
    return jnp.sum(jnp.where(eye, row, 0.0), axis=1, keepdims=True)


def kernel(
    n_pix, n_par, green, observed, sol_out, res_out,
    gmat, grad, near_send, near_recv, near_low, near_low_recv, own_part, wide_send, wide_recv,
    wide_low, wide_low_recv, rows_near, rows_wide,
    near_grad, halo, direction, smooth1, smooth2, solution, residual, image, image_bf,
    partial, pair_recv, chip_buf, half_send, half_recv, fresh_rows, smooth_rows, final_rows, row_send,
    ratio_buf,
    g_sem, as_sem, ar_sem, bs_sem, br_sem, cs_sem, cr_sem, hs_sem, hr_sem, xs_sem, x1r_sem, x2r_sem,
    x3r_sem, fs_sem, fr_sem, ss_sem, sr_sem, zs_sem, zr_sem, ars_sem, arr_sem, brs_sem, brr_sem,
    als_sem, alr_sem, bls_sem, blr_sem,
):
    sets = observed.shape[0]
    pixels = observed.shape[1]
    chunk = gmat.shape[2]
    rows_per = chunk // GRID
    blocks = n_pix // WINDOW
    rows = direction.shape[0] - 2 * rows_per
    half = sets // 2
    z = lax.axis_index("pix")
    par = lax.axis_index("par")
    core = lax.rem(par, 2)
    chip = lax.div(par, 2)
    chips = n_par // 2
    mate = par + 1 - 2 * core
    own_class = lax.rem(z, WINDOW)
    own_block = lax.div(z, WINDOW)
    early = jnp.where(z < n_pix // 2, 1, blocks - 1)
    tiles = pixels // GRID
    edge = (tiles + 1) // 2 * GRID
    parts = ((0, edge), (edge, pixels - edge))

    def at_pix(offset):
        return {"pix": lax.rem(z + (offset + n_pix), n_pix)}

    def at_par(offset):
        return {"par": lax.rem(par + offset, n_par)}

    def class_at(offset):
        return lax.rem(z + (offset + n_pix), WINDOW)

    def remote(src, dst, send, recv, device):
        return pltpu.make_async_remote_copy(
            src_ref=src, dst_ref=dst, send_sem=send, recv_sem=recv, device_id=device, device_id_type=MESH
        )

    def matrix_load(index, offset):
        place = class_at(offset)
        columns = pl.ds(pl.multiple_of(place * chunk, chunk), chunk)
        return pltpu.make_async_copy(green.at[:, columns], gmat.at[place], g_sem.at[index])

    for index, offset in enumerate(NEAR + (0,)):
        matrix_load(index, offset).start()

    halo[...] = jnp.zeros_like(halo)
    smooth_rows[...] = jnp.zeros_like(smooth_rows)
    barrier = pltpu.get_barrier_semaphore()
    for offset in range(1, WINDOW // 2 + 1):
        for place in (offset, -offset):
            pl.semaphore_signal(barrier, inc=1, device_id=at_pix(place), device_id_type=MESH)
    for offset in range(1, n_par):
        pl.semaphore_signal(barrier, inc=1, device_id=at_par(offset), device_id_type=MESH)

    lane = lax.broadcasted_iota(jnp.int32, (sets, GRID), 1)
    eye = lane == lax.broadcasted_iota(jnp.int32, (sets, GRID), 0)
    first_lane = lane == 0
    last_lane = lane == GRID - 1

    direction[...] = jnp.zeros_like(direction)
    smooth2[...] = jnp.zeros_like(smooth2)
    smooth1[...] = jnp.zeros_like(smooth1)
    solution[...] = jnp.zeros_like(solution)
    image[...] = jnp.zeros_like(image)
    grad[...] = jnp.zeros_like(grad)
    image_bf[...] = observed[...]
    residual[...] = observed[...].astype(F32)
    pl.semaphore_wait(barrier, WINDOW + n_par - 1)

    def all_par(rows_ref, row, slot_sem, send_sem, index):
        row_send[index] = row
        rows_ref[par] = row
        for offset in range(1, n_par):
            remote(
                row_send.at[index], rows_ref.at[par], send_sem, slot_sem, at_par(offset)
            ).start()

    def wait_rows(rows_ref, sem, count):
        part = rows_ref.at[pl.ds(0, count)]
        remote(part, part, sem, sem, at_par(1)).wait_recv()

    def neighbours_sum(field, row):
        here = field[row]
        left = jnp.where(first_lane, 0.0, pltpu.roll(here, 1, 1))
        right = jnp.where(last_lane, 0.0, pltpu.roll(here, GRID - 1, 1))
        return here, left + right

    def sum_par(rows_ref):
        total = rows_ref[0]
        for index in range(1, n_par):
            total = total + rows_ref[index]
        return total

    def send_near(source, target, slot, offset, send, recv):
        if offset == WINDOW // 2:
            for part, place in enumerate((offset, -offset)):
                cut = pl.ds(part * half, half)
                remote(
                    source.at[slot, cut], target.at[slot, cut], send, recv, at_pix(place)
                ).start()
        else:
            remote(source.at[slot], target.at[slot], send, recv, at_pix(offset)).start()

    def sweep_body(sweep, grad_sq):
        parity = lax.rem(sweep, 2)
        started = sweep > 0
        first = sweep == 0

        lhs = image_bf[...]
        for slot, offset in enumerate(NEAR):

            @pl.when(first)
            def _():
                matrix_load(slot, offset).wait()

            product = jnp.dot(lhs, gmat[class_at(offset)], preferred_element_type=F32)
            rounded = product.astype(BF16)
            near_send[slot] = rounded
            send_near(near_send, near_recv, slot, offset, as_sem, ar_sem)

            @pl.when(first)
            def _():
                near_low[slot] = (product - rounded.astype(F32)).astype(BF16)
                send_near(near_low, near_low_recv, slot, offset, als_sem, alr_sem)

            if slot == 1:
                value = image[...]
                image_row = row_sums(value * value, eye)
                row_send[2] = image_row
                rows_near[len(NEAR)] = image_row
                for place, target in enumerate(NEAR):
                    remote(
                        row_send.at[2], rows_near.at[place], ars_sem, arr_sem, at_pix(target)
                    ).start()

        @pl.when(first)
        def _():
            matrix_load(len(NEAR), 0).wait()

        total = jnp.dot(lhs, gmat[own_class], preferred_element_type=F32)
        remote(near_recv, near_recv, ar_sem, ar_sem, at_pix(1)).wait_recv()
        for slot in range(len(NEAR)):
            total = total + near_recv[slot].astype(F32)
        own_part[...] = total

        @pl.when(first)
        def _():
            remote(near_low_recv, near_low_recv, als_sem, alr_sem, at_pix(1)).wait_recv()
            more = near_low_recv[0].astype(F32)
            for slot in range(1, len(NEAR)):
                more = more + near_low_recv[slot].astype(F32)
            own_part[...] += more

        total = own_part[...]
        rounded = total.astype(BF16)
        wide_send[...] = rounded
        wide_recv[parity, 0] = rounded
        middle = blocks // 2
        sides = [b for b in range(1, blocks) if b != middle]

        def send_wide(block):
            slot = blocks - block
            remote(
                wide_send, wide_recv.at[parity, slot], bs_sem, br_sem.at[parity, slot],
                at_pix(block * WINDOW),
            ).start()

        def wait_wide(slot):
            part = wide_recv.at[parity, slot]
            remote(part, part, bs_sem, br_sem.at[parity, slot], at_pix(1)).wait_recv()

        def send_rows(block):
            remote(
                rows_wide.at[parity, 0], rows_wide.at[parity, blocks - block], brs_sem,
                brr_sem.at[parity], at_pix(block * WINDOW),
            ).start()

        @pl.when(started)
        def _():
            send_wide(middle)

        for block in sides:
            send_wide(block)
        part = rows_near.at[pl.ds(0, len(NEAR))]
        remote(part, part, arr_sem, arr_sem, at_pix(1)).wait_recv()
        for slot in range(WINDOW):
            rows_wide[parity, 0, slot] = rows_near[slot]
        for block in sides:
            send_rows(block)

        @pl.when(first)
        def _():
            low_part = (total - rounded.astype(F32)).astype(BF16)
            wide_low[...] = low_part
            wide_low_recv[0] = low_part
            wait_wide(early)
            send_wide(middle)
            for block in [middle] + sides:
                remote(
                    wide_low, wide_low_recv.at[blocks - block], bls_sem, blr_sem,
                    at_pix(block * WINDOW),
                ).start()

        send_rows(middle)

        @pl.when(started)
        def _():
            wait_rows(smooth_rows, sr_sem, n_par - 1)

        smooth_sq = sum_par(smooth_rows)

        part = rows_wide.at[parity, pl.ds(0, blocks - 1)]
        remote(part, part, brs_sem, brr_sem.at[parity], at_pix(1)).wait_recv()
        image_sq = canonical_rows(parity)
        step_row = jnp.where(started, grad_sq / (image_sq + smooth_sq), -1.0)
        step = to_column(step_row, eye)

        @pl.when(started)
        def _():
            wait_wide(early)

        wait_wide(blocks - early)
        wait_wide(middle)
        total = None
        for block in range(blocks):
            term = wide_recv[parity, lax.rem(block - own_block + blocks, blocks)].astype(F32)
            total = term if total is None else total + term
        own_part[...] = total

        @pl.when(first)
        def _():
            part = wide_low_recv.at[pl.ds(0, blocks - 1)]
            remote(part, part, bls_sem, blr_sem, at_pix(1)).wait_recv()
            more = None
            for block in range(blocks):
                place = lax.rem(block - own_block + blocks, blocks)
                term = wide_low_recv[place].astype(F32)
                more = term if more is None else more + term
            own_part[...] += more
            remote(near_low, near_low, als_sem, alr_sem, at_pix(1)).wait_send()
            remote(part, part, bls_sem, blr_sem, at_pix(1)).wait_send()

        total = own_part[...]
        for index in range(rows_per):
            cut = slice(index * GRID, (index + 1) * GRID)
            full = total[:, cut] + smooth2[own_class * rows_per + index]
            grad[:, cut] = grad[:, cut] - step * full
        rounded = grad[...].astype(BF16)
        near_grad[own_class] = rounded
        for offset in NEAR:
            if offset == WINDOW // 2:
                for part, place in enumerate((-offset, offset)):
                    piece = near_grad.at[own_class, pl.ds(part * half, half)]
                    remote(piece, piece, cs_sem, cr_sem.at[offset + 3], at_pix(place)).start()
            else:
                piece = near_grad.at[own_class]
                remote(piece, piece, cs_sem, cr_sem.at[offset + 3], at_pix(-offset)).start()

        residual[...] = residual[...] - step * image[...]

        def columns_image(block, index, start, size):
            return lax.dot_general(
                block, gmat[index, start : start + size], (((1,), (1,)), ((), ())),
                preferred_element_type=F32,
            )

        block = near_grad[own_class]
        partial[...] = columns_image(block, own_class, 0, pixels)
        value = block.astype(F32)
        squares = value * value
        my_rows = pl.ds(pl.multiple_of(core * half, half), half)
        their_rows = pl.ds(pl.multiple_of((1 - core) * half, half), half)

        def pair_copy(index):
            start, size = parts[index]
            cut = pl.ds(start, size)
            return remote(
                partial.at[their_rows, cut], pair_recv.at[:, cut], xs_sem.at[0, index],
                x1r_sem.at[index], {"par": mate},
            )

        def back_copy(index):
            start, size = parts[index]
            cut = pl.ds(start, size)
            return remote(
                half_send.at[:, cut], half_recv.at[:, cut], xs_sem.at[1, index],
                x3r_sem.at[index], {"par": mate},
            )

        arrivals = (1, -1, 2, -2, 3, -3, 4)
        for offset in arrivals:
            place = class_at(offset)
            remote(
                near_grad.at[0], near_grad.at[0], cs_sem, cr_sem.at[offset + 3], at_pix(1)
            ).wait_recv()
            block = near_grad[place]
            if offset == arrivals[-1]:
                for index, (start, size) in enumerate(parts):
                    partial[:, start : start + size] += columns_image(block, place, start, size)
                    pair_copy(index).start()
            else:
                partial[...] += columns_image(block, place, 0, pixels)
            value = block.astype(F32)
            squares = squares + value * value
        all_par(fresh_rows, row_sums(squares, eye), fr_sem, fs_sem, 0)

        low = remote(near_grad.at[0], halo.at[1], hs_sem.at[0], hr_sem.at[1], {"par": lax.rem(par + n_par - 1, n_par)})
        high = remote(near_grad.at[WINDOW - 1], halo.at[0], hs_sem.at[1], hr_sem.at[0], at_par(1))

        @pl.when(par > 0)
        def _():
            low.start()

        @pl.when(par < n_par - 1)
        def _():
            high.start()

        for index, (start, size) in enumerate(parts):
            cut = slice(start, start + size)
            pair_copy(index).wait_recv()
            mine = partial[my_rows, cut] + pair_recv[:, cut]
            chip_buf[parity, chip, :, cut] = mine.astype(BF16)
            piece = chip_buf.at[parity, chip, :, pl.ds(start, size)]
            for offset in (2, 1, 3):
                remote(
                    piece, piece, xs_sem.at[2, index], x2r_sem.at[parity, index], at_par(2 * offset)
                ).start()

        wait_rows(fresh_rows, fr_sem, n_par - 1)
        fresh_sq = sum_par(fresh_rows)
        ratio_row = jnp.where(started, fresh_sq / grad_sq, 0.0)
        ratio = to_column(ratio_row, eye)
        ratio_buf[...] = jnp.broadcast_to(ratio, ratio_buf.shape)
        for row in range(rows):
            old = direction[row + rows_per]
            solution[row] = solution[row] + step * old
            cut = slice(row % rows_per * GRID, (row % rows_per + 1) * GRID)
            new = near_grad[row // rows_per, :, cut].astype(F32)
            direction[row + rows_per] = new + ratio * old

        @pl.when(par < n_par - 1)
        def _():
            low.wait_recv()

        @pl.when(par > 0)
        def _():
            high.wait_recv()

        for index in range(rows_per):
            cut = slice(index * GRID, (index + 1) * GRID)
            direction[index] = halo[0, :, cut].astype(F32) + ratio * direction[index]
            top = rows + rows_per + index
            direction[top] = halo[1, :, cut].astype(F32) + ratio * direction[top]

        squares = None
        for row in range(rows + 2):
            here, beside = neighbours_sum(direction, row + rows_per - 1)
            beside = beside + direction[row + rows_per - 2] + direction[row + rows_per]
            value = here - 0.25 * beside
            if row == 0:
                value = jnp.where(par > 0, value, 0.0)
            elif row == rows + 1:
                value = jnp.where(par < n_par - 1, value, 0.0)
            else:
                squares = value * value if squares is None else squares + value * value
            smooth1[row] = value
        all_par(smooth_rows, row_sums(squares, eye), sr_sem, ss_sem, 1)
        for row in range(rows):
            here, beside = neighbours_sum(smooth1, row + 1)
            smooth2[row] = here - 0.25 * (beside + smooth1[row] + smooth1[row + 2])

        def chip_parts(index):
            start, size = parts[index]
            return chip_buf.at[parity, pl.ds(0, chips - 1), :, pl.ds(start, size)]

        for index, (start, size) in enumerate(parts):
            cut = slice(start, start + size)
            part = chip_parts(index)
            remote(
                part, part, xs_sem.at[2, index], x2r_sem.at[parity, index], at_par(1)
            ).wait_recv()
            total = chip_buf[parity, 0, :, cut].astype(F32)
            for other in range(1, chips):
                total = total + chip_buf[parity, other, :, cut].astype(F32)
            half_send[:, cut] = total
            back_copy(index).start()
            value = total + ratio_buf[my_rows, 0:1] * image[my_rows, cut]
            image[my_rows, cut] = value
            image_bf[my_rows, cut] = value.astype(BF16)
        for index, (start, size) in enumerate(parts):
            cut = slice(start, start + size)
            back_copy(index).wait_recv()
            value = half_recv[:, cut] + ratio_buf[their_rows, 0:1] * image[their_rows, cut]
            image[their_rows, cut] = value
            image_bf[their_rows, cut] = value.astype(BF16)

        remote(near_send, near_send, as_sem, as_sem, at_pix(1)).wait_send()
        part = rows_near.at[pl.ds(0, len(NEAR))]
        remote(part, part, ars_sem, ars_sem, at_pix(1)).wait_send()
        part = wide_recv.at[parity, pl.ds(0, blocks - 1)]
        remote(part, part, bs_sem, bs_sem, at_pix(1)).wait_send()
        part = rows_wide.at[parity, pl.ds(0, blocks - 1)]
        remote(part, part, brs_sem, brs_sem, at_pix(1)).wait_send()
        remote(near_send, near_send, cs_sem, cs_sem, at_pix(1)).wait_send()
        part = fresh_rows.at[pl.ds(0, n_par - 1)]
        remote(part, part, fs_sem, fs_sem, at_pix(1)).wait_send()
        remote(part, part, ss_sem, ss_sem, at_pix(1)).wait_send()
        for index in range(len(parts)):
            part = chip_parts(index)
            remote(
                part, part, xs_sem.at[2, index], x2r_sem.at[parity, index], at_par(1)
            ).wait_send()
            pair_copy(index).wait_send()
            back_copy(index).wait_send()

        @pl.when(par > 0)
        def _():
            low.wait_send()

        @pl.when(par < n_par - 1)
        def _():
            high.wait_send()

        return fresh_sq

    def canonical_rows(parity):
        total = None
        for shard in range(n_pix):
            back = lax.rem(shard - z + (2 * n_pix + WINDOW // 2), n_pix)
            block = lax.div(back, WINDOW)
            inside = lax.rem(back, WINDOW)
            row = rows_wide[parity, block, slot_of(inside)]
            total = row if total is None else total + row
        return total

    def slot_of(inside):
        offset = WINDOW // 2 - inside
        slot = len(NEAR)
        for index, value in enumerate(NEAR):
            slot = jnp.where(offset == value, index, slot)
        return slot

    grad_sq = lax.fori_loop(0, ITERS, sweep_body, jnp.zeros((1, GRID), F32))

    value = image[...]
    image_row = row_sums(value * value, eye)
    row_send[2] = image_row
    final_rows[z] = image_row
    for offset in [s * d for d in range(n_pix // 2, 0, -1) for s in (1, -1)][1:]:
        remote(row_send.at[2], final_rows.at[z], zs_sem, zr_sem, at_pix(offset)).start()
    wait_rows(smooth_rows, sr_sem, n_par - 1)
    smooth_sq = sum_par(smooth_rows)
    part = final_rows.at[pl.ds(0, n_pix - 1)]
    remote(part, part, zs_sem, zr_sem, at_pix(1)).wait_recv()
    image_sq = final_rows[0]
    for shard in range(1, n_pix):
        image_sq = image_sq + final_rows[shard]
    step = to_column(grad_sq / (image_sq + smooth_sq), eye)
    for row in range(rows):
        sol_out[:, row * GRID : (row + 1) * GRID] = solution[row] + step * direction[row + rows_per]
    res_out[...] = residual[...] - step * image[...]
    remote(part, part, zs_sem, zs_sem, at_pix(1)).wait_send()


def solution(mesh):
    n_pix, n_par = mesh.shape["pix"], mesh.shape["par"]

    def on_device(green_matrix, observed):
        pixels, cells = green_matrix.shape
        sets = observed.shape[0]
        chunk = cells // WINDOW
        rows = cells // GRID
        extra = chunk // GRID
        blocks = n_pix // WINDOW
        half = sets // 2
        near = len(NEAR)
        dma = pltpu.SemaphoreType.DMA
        vmem = pltpu.VMEM
        return pl.pallas_call(
            functools.partial(kernel, n_pix, n_par),
            out_shape=(
                jax.ShapeDtypeStruct((sets, cells), F32),
                jax.ShapeDtypeStruct((sets, pixels), F32),
            ),
            in_specs=[
                pl.BlockSpec(memory_space=pl.ANY),
                pl.BlockSpec(memory_space=pltpu.VMEM),
            ],
            out_specs=(
                pl.BlockSpec(memory_space=pltpu.VMEM),
                pl.BlockSpec(memory_space=pltpu.VMEM),
            ),
            scratch_shapes=[
                vmem((WINDOW, pixels, chunk), BF16),
                vmem((sets, chunk), F32),
                vmem((near, sets, chunk), BF16),
                vmem((near, sets, chunk), BF16),
                vmem((near, sets, chunk), BF16),
                vmem((near, sets, chunk), BF16),
                vmem((sets, chunk), F32),
                vmem((sets, chunk), BF16),
                vmem((2, blocks, sets, chunk), BF16),
                vmem((sets, chunk), BF16),
                vmem((blocks, sets, chunk), BF16),
                vmem((WINDOW, 1, GRID), F32),
                vmem((2, blocks, WINDOW, 1, GRID), F32),
                vmem((WINDOW, sets, chunk), BF16),
                vmem((2, sets, chunk), BF16),
                vmem((rows + 2 * extra, sets, GRID), F32),
                vmem((rows + 2, sets, GRID), F32),
                vmem((rows, sets, GRID), F32),
                vmem((rows, sets, GRID), F32),
                vmem((sets, pixels), F32),
                vmem((sets, pixels), F32),
                vmem((sets, pixels), BF16),
                vmem((sets, pixels), F32),
                vmem((half, pixels), F32),
                vmem((2, n_par // 2, half, pixels), BF16),
                vmem((half, pixels), F32),
                vmem((half, pixels), F32),
                vmem((n_par, 1, GRID), F32),
                vmem((n_par, 1, GRID), F32),
                vmem((n_pix, 1, GRID), F32),
                vmem((3, 1, GRID), F32),
                vmem((sets, GRID), F32),
                dma((WINDOW,)),
                dma, dma,
                dma, dma((2, blocks)),
                dma, dma((WINDOW,)),
                dma((2,)), dma((2,)),
                dma((3, 2)), dma((2,)), dma((2, 2)), dma((2,)),
                dma, dma,
                dma, dma,
                dma, dma,
                dma, dma,
                dma, dma((2,)),
                dma, dma, dma, dma,
            ],
            compiler_params=pltpu.CompilerParams(collective_id=0, has_side_effects=True),
        )(green_matrix, observed)

    return jax.shard_map(
        on_device,
        mesh=mesh,
        in_specs=(P("pix", "par"), P("parts", "pix")),
        out_specs=(P("parts", "par"), P("parts", "pix")),
        check_vma=False,
    )
```
